256 devices in a mesh: dp: 8 (over x, y_lo), tp: 32 (over y_hi, z, core).
Axes of the slice: x: 4, y: 4 (y_hi: 2, y_lo: 2; y = y_hi * 2 + y_lo), z: 8, core: 2. Of those that a mesh axis runs over, the one named last changes fastest.
Arguments:
- proj_in: bfloat16 [1, 32768, 8192], P(None, 'dp', 'tp'), may hold values from -6 to 6
- kv_grad: bfloat16 [1, 32768, 2048], P(None, ('dp', 'tp')), may hold values from -0.75 to 0.75
- normed: bfloat16 [1, 32768, 8192], P(None, ('dp', 'tp')), may hold values from -6 to 6
- norm_grad: bfloat16 [1, 32768, 8192], P(None, ('dp', 'tp')), may hold values from -0.6 to 0.6
- first_moment: float32 [1, 8192, 2048], P(None, 'tp', 'dp'), may hold values from -0.6 to 0.6
- second_moment: float32 [1, 8192, 2048], P(None, 'tp', 'dp'), may hold values from 0.002 to 0.02
Outputs:
- new_first: float32 [1, 8192, 2048], P(None, 'tp', 'dp')
- new_second: float32 [1, 8192, 2048], P(None, 'tp', 'dp')
- adam_step: float32 [1, 8192, 2048], P(None, 'tp', 'dp')
- gain_grad: float32 [1, 8192], replicated
The draws below stay inside these ranges and needn't reach their ends.
All inputs are finite; a program needn't handle non-finite values.
Results may differ from the reference program's by a relative error of at most 0.0003.
Values may be sent and summed in bfloat16 or wider, within the bound.
A program may use at most 128 MiB of HBM per device.

```python
import math
import jax
import jax.numpy as jnp
from jax import lax

D = 8192
KV = 2048
LAYERS = 1
TOK_REP = 4096
TOKENS = 32768
N_DP = 8


def draw_norm_grad(key, part):
    first_key, second_key, third_key = jax.random.split(key, 3)
    values = 0.1 * jax.random.normal(first_key, (LAYERS, TOKENS, D), jnp.float32)
    return jnp.clip(values, -0.6, 0.6).astype(jnp.bfloat16)


def strengthened(result, own_key, source, target, parts, factor):
    def block_of(position):
        return (jnp.arange(result.shape[position]) // (result.shape[position] // parts)).reshape((-1,) + (1,) * (result.ndim - 1 - position))

    one_side = jax.random.permutation(own_key, parts)[block_of(target)]
    second = (block_of(target) + parts // 2) % parts
    return jnp.where((block_of(source) == one_side) | (block_of(source) == second), factor * result, result)


def block_levels(stream_key, dims, shards, least, top_value):
    factor_of, own = 1.0, jax.random.fold_in(stream_key, 6)
    for axis_at, parts in shards:
        draws = jnp.exp(jax.random.uniform(jax.random.fold_in(own, axis_at), (parts,), jnp.float32, least / len(shards), top_value / len(shards)))
        factor_of = factor_of * jnp.repeat(draws, dims[axis_at] // parts).reshape([-1 if axis == axis_at else 1 for axis in range(len(dims))])
    return factor_of


def bell_draw(rng, extent, scale, bound, pieces=(), held_as=jnp.bfloat16):
    loudness = block_levels(rng, extent, pieces, -0.22, 0.18) if pieces else 1.0
    array = jax.random.normal(rng, extent, jnp.float32) * scale * loudness
    return jnp.minimum(jnp.maximum(array, -bound), bound).astype(held_as)


def heavy_noise(key, shape, deviation, limit, cuts, heavy, held_as=jnp.bfloat16):
    drawn = deviation * jax.random.normal(key, shape, jnp.float32)
    if cuts:
        drawn = drawn * block_levels(key, shape, cuts, -0.22, 0.18)
    return jnp.clip(strengthened(drawn, jax.random.fold_in(key, 3), *heavy), -limit, limit).astype(held_as)


def setup_inputs(seed: int = 0) -> dict:
    splits = jax.random.split(jax.random.key(seed), 7)
    return {
        "proj_in": bell_draw(splits[0], (LAYERS, TOKENS, D), 1.0, 6.0, ((1, 8), (2, 32))),
        "kv_grad": heavy_noise(splits[1], (LAYERS, TOKENS, KV), 0.03, 0.75, ((1, 256),), (1, 2, 256, 6.0)),
        "normed": bell_draw(splits[2], (LAYERS, TOKENS, D), 1.0, 6.0, ((1, 256),)),
        "norm_grad": draw_norm_grad(jax.random.fold_in(splits[6], 71), 0),
        "first_moment": bell_draw(splits[4], (LAYERS, D, KV), 0.1, 0.6, ((1, 32), (2, 8)), jnp.float32),
        "second_moment": jnp.clip(jnp.exp(math.log(0.02) - 2.30258502 * jax.random.uniform(splits[5], (LAYERS, D, KV), jnp.float32) ** block_levels(splits[5], (LAYERS, D, KV), ((1, 32), (2, 8)), -0.2, 0.2)), 0.002, 0.02),
    }


beta_one = 0.9
beta_two = 0.95
correct_one = 0.19
correct_two = 0.0975
epsilon = 1e-08

def reference(proj_in, kv_grad, normed, norm_grad, first_moment, second_moment):
    firsts = []
    seconds = []
    updates = []
    for layer_id in range(LAYERS):
        running = jnp.zeros((D, KV), jnp.float32)
        for replica in range(N_DP):
            inputs = proj_in[layer_id, replica * TOK_REP:(replica + 1) * TOK_REP]
            grad_rows = kv_grad[layer_id, replica * TOK_REP:(replica + 1) * TOK_REP]
            product = lax.dot_general(inputs, grad_rows, (((0,), (0,)), ((), ())), preferred_element_type=jnp.float32)
            running = running + product
        mean_grad = running / N_DP
        new_first = beta_one * first_moment[layer_id] + (1.0 - beta_one) * mean_grad
        new_second = beta_two * second_moment[layer_id] + (1.0 - beta_two) * mean_grad * mean_grad
        update = new_first / correct_one / (jnp.sqrt(new_second / correct_two) + epsilon)
        firsts.append(new_first)
        seconds.append(new_second)
        updates.append(update)
    gain_grad = lax.optimization_barrier(jnp.sum(norm_grad.astype(jnp.float32) * normed.astype(jnp.float32), axis=1)) / N_DP
    return (jnp.stack(firsts), jnp.stack(seconds), jnp.stack(updates), gain_grad)
```

```python
import functools

import jax
import jax.numpy as jnp
from jax import lax
from jax.experimental import pallas as pl
from jax.experimental.pallas import tpu as pltpu
from jax.sharding import Mesh
from jax.sharding import PartitionSpec as P

X, YLO, YHI, Z, CORE = "dp_0", "dp_1", "tp_0", "tp_1", "tp_2"
DP = (X, YLO)
TP = (YHI, Z, CORE)
DP_TP = DP + TP
MESH = pl.DeviceIdType.MESH

beta_one = 0.9
beta_two = 0.95
correct_one = 0.19
correct_two = 0.0975
epsilon = 1e-08

ORDER = (
    ('XS',), ('S', 0), ('S', 1), ('XO', 0), ('XO', 1), ('XO', 2), ('XO', 3), ('GC',), ('E', 0, 1), ('R', 0), ('GX',),
    ('E', 1, 1), ('R', 1), ('GY',), ('E', 0, 2), ('R', 2), ('E', 1, 2), ('R', 3), ('E', 0, 3), ('XA', 0), ('S', 2),
    ('E', 1, 3), ('XA', 1), ('E', 0, 4), ('GZ',), ('M', 0, 0), ('E', 2, 1), ('XA', 2), ('E', 1, 4), ('GA',),
    ('M', 1, 0), ('XA', 3), ('X1', 0, 0), ('M', 0, 1), ('E', 2, 2), ('M', 1, 1), ('GO',), ('X1', 1, 0), ('S', 3),
    ('X2', 0, 0), ('E', 2, 3), ('X1', 0, 1), ('E', 3, 1), ('X1', 1, 1), ('E', 2, 4), ('M', 2, 0), ('X2', 1, 0),
    ('M', 2, 1), ('E', 3, 2), ('X2', 0, 1), ('X2', 1, 1), ('X1', 2, 0), ('Y1', 0, 0), ('Y1', 0, 1), ('E', 3, 3),
    ('X1', 2, 1), ('Y1', 1, 0), ('Y1', 1, 1), ('X2', 2, 0), ('E', 3, 4), ('Y2', 0), ('X2', 2, 1), ('M', 3, 0),
    ('M', 3, 1), ('Y2', 1), ('Y1', 2, 0), ('X1', 3, 0), ('Y1', 2, 1), ('X1', 3, 1), ('Y2', 2), ('X2', 3, 0),
    ('X2', 3, 1), ('Y1', 3, 0), ('Y1', 3, 1), ('Y2', 3),
)


def adam_update(mean_grad, first_old, second_old):
    new_first = beta_one * first_old + (1.0 - beta_one) * mean_grad
    new_second = beta_two * second_old + (1.0 - beta_two) * mean_grad * mean_grad
    update = new_first / correct_one / (jnp.sqrt(new_second / correct_two) + epsilon)
    return (new_first, new_second, update)


SCRATCH = dict(
    gbuf=pltpu.VMEM((4, 8, 2, 128, 512), jnp.bfloat16),
    xown=pltpu.VMEM((2048, 256), jnp.bfloat16),
    xoth=pltpu.VMEM((2, 4, 256, 256), jnp.bfloat16),
    relay=pltpu.VMEM((2, 4, 256, 256), jnp.bfloat16),
    xt=pltpu.VMEM((2, 256, 2048), jnp.bfloat16),
    part=pltpu.VMEM((4, 2, 4, 256, 128), jnp.float32),
    xfar=pltpu.VMEM((4, 2, 2, 128, 128), jnp.float32),
    xnear=pltpu.VMEM((4, 2, 2, 256, 128), jnp.float32),
    summed=pltpu.VMEM((4, 2, 256, 128), jnp.float32),
    yfar=pltpu.VMEM((4, 2, 128, 128), jnp.float32),
    ynear=pltpu.VMEM((4, 2, 256, 128), jnp.float32),
    nbuf=pltpu.VMEM((128, 8192), jnp.bfloat16),
    ngbuf=pltpu.VMEM((128, 8192), jnp.bfloat16),
    gain_c=pltpu.VMEM((2, 8, 8, 128), jnp.float32),
    gain_x=pltpu.VMEM((4, 8, 8, 128), jnp.float32),
    gain_y=pltpu.VMEM((4, 8, 8, 128), jnp.float32),
    gain_s=pltpu.VMEM((8, 8, 128), jnp.float32),
    gain_z=pltpu.VMEM((8, 8, 128), jnp.float32),
    gain_a=pltpu.VMEM((8, 8, 128), jnp.float32),
    load=pltpu.SemaphoreType.DMA((7,)),
    z_s=pltpu.SemaphoreType.DMA((4, 2, 4)),
    z_r=pltpu.SemaphoreType.DMA((4, 2, 4)),
    d_s=pltpu.SemaphoreType.DMA((4, 9)),
    d_r=pltpu.SemaphoreType.DMA((4, 9)),
    x1_s=pltpu.SemaphoreType.DMA((2, 4)),
    x1_r=pltpu.SemaphoreType.DMA((2, 4)),
    x2_s=pltpu.SemaphoreType.DMA((2, 4)),
    x2_r=pltpu.SemaphoreType.DMA((2, 4)),
    u_s=pltpu.SemaphoreType.DMA((4, 2, 6)),
    u_r=pltpu.SemaphoreType.DMA((4, 2, 6)),
    y_s=pltpu.SemaphoreType.DMA((4, 2, 2)),
    yf_r=pltpu.SemaphoreType.DMA((4, 2)),
    yn_r=pltpu.SemaphoreType.DMA((4, 2, 2)),
    g_s=pltpu.SemaphoreType.DMA((21,)),
    g_r=pltpu.SemaphoreType.DMA((21,)),
)


def exchange(x_hbm, g_hbm, n_hbm, ng_hbm, out_ref, gain_ref, *scratch):
    b = dict(zip(SCRATCH, scratch, strict=True))
    x, ylo, yhi = lax.axis_index(X), lax.axis_index(YLO), lax.axis_index(YHI)
    z, core = lax.axis_index(Z), lax.axis_index(CORE)
    y = yhi * 2 + ylo
    other = 1 - core

    def ring(value, size):
        return lax.rem(value + size, size)

    def at_x(step):
        return {X: ring(x + step, 4)}

    def at_y(step):
        there = ring(y + step, 4)
        return {YHI: there // 2, YLO: lax.rem(there, 2)}

    def at_z(step):
        return {Z: ring(z + step, 8)}

    sibling = {CORE: other}
    both = (1, -1)
    sent = []

    def copy(src, dst, send, recv, to):
        return pltpu.make_async_remote_copy(
            src_ref=src, dst_ref=dst, send_sem=send, recv_sem=recv, device_id=to, device_id_type=MESH
        )

    def start(*args):
        made = copy(*args)
        made.start()
        sent.append(made)

    loads = []
    for j in range(4):
        for k in range(4):
            first = k * 512 + (j % 2) * 256 + (j // 2) * 128
            loads.append(
                pltpu.make_async_copy(
                    g_hbm.at[:, pl.ds(first, 128)],
                    b["gbuf"].at[j, z, core, :, pl.ds(k * 128, 128)],
                    b["load"].at[j],
                )
            )
    own_rows = pl.multiple_of(yhi * 2048, 2048)
    away_rows = pl.multiple_of((1 - yhi) * 2048, 2048)
    load_x = pltpu.make_async_copy(x_hbm.at[pl.ds(own_rows, 2048), :], b["xown"], b["load"].at[4])
    load_n = pltpu.make_async_copy(n_hbm, b["nbuf"], b["load"].at[5])
    load_ng = pltpu.make_async_copy(ng_hbm, b["ngbuf"], b["load"].at[6])
    for one in loads:
        one.start()
    load_x.start()
    load_n.start()
    load_ng.start()

    barrier = pltpu.get_barrier_semaphore()
    greeted = [sibling]
    greeted += [at_x(k) for k in range(1, 4)] + [at_y(k) for k in range(1, 4)] + [at_z(k) for k in range(1, 8)]
    for peer in greeted:
        pl.semaphore_signal(barrier, inc=1, device_id=peer, device_id_type=MESH)
    pl.semaphore_wait(barrier, len(greeted))

    def z_copy(j, d, s, arriving):
        hops = s if arriving else s - 1
        source = ring(z - hops * both[d], 8)
        piece = b["gbuf"].at[j, source, core]
        if s == 4:
            piece = piece.at[pl.ds(64 * d, 64)]
        return piece, piece, b["z_s"].at[j, d, s - 1], b["z_r"].at[j, d, s - 1], at_z(both[d])

    def d_copy(j, d, s, half):
        source = z if s == 0 else ring(z - s * both[d], 8)
        piece = b["gbuf"].at[j, source, half]
        if s == 4:
            piece = piece.at[pl.ds(64 * d, 64)]
        slot = 0 if s == 0 else d * 4 + s
        return piece, piece, b["d_s"].at[j, slot], b["d_r"].at[j, slot], sibling

    def S(j):
        pltpu.make_async_copy(b["gbuf"].at[j, z, core], b["gbuf"].at[j, z, core], b["load"].at[j]).wait()
        for d in range(2):
            start(*z_copy(j, d, 1, False))
        start(*d_copy(j, 0, 0, core))

    def E(j, s):
        for d in range(2):
            copy(*z_copy(j, d, s, True)).wait_recv()
            if s < 4:
                start(*z_copy(j, d, s + 1, False))
            start(*d_copy(j, d, s, core))

    def relay_copy(d, m):
        rows = pl.multiple_of(away_rows + d * 1024 + m * 256, 256)
        return x_hbm.at[pl.ds(rows, 256), :], b["relay"].at[d, m], b["x1_s"].at[d, m], b["x1_r"].at[d, m], at_y(both[d])

    def onward_copy(d, m):
        return b["relay"].at[d, m], b["xoth"].at[d, m], b["x2_s"].at[d, m], b["x2_r"].at[d, m], at_y(both[d])

    def XS():
        for m in range(4):
            for d in range(2):
                start(*relay_copy(d, m))

    def R(m):
        for d in range(2):
            copy(*relay_copy(d, m)).wait_recv()
            start(*onward_copy(d, m))

    def XO(m):
        if m == 0:
            load_x.wait()
        for k in (2 * m, 2 * m + 1):
            b["xt"][0, :, k * 256 : (k + 1) * 256] = b["xown"][k * 256 : (k + 1) * 256, :].T

    def XA(m):
        for d in range(2):
            copy(*onward_copy(d, m)).wait_recv()
            k = d * 4 + m
            b["xt"][1, :, k * 256 : (k + 1) * 256] = b["xoth"][d, m].T

    def peers(at, me, count, buf, first, source=None):
        made = []
        for k in range(1, count):
            src = buf.at[me] if source is None else source.at[ring(me + k, count)]
            dst = buf.at[me]
            made.append((src, dst, b["g_s"].at[first + k - 1], b["g_r"].at[first + k - 1], at(k)))
        return made

    def arrived(me, count, buf, first, at):
        for k in range(1, count):
            piece = buf.at[ring(me - k, count)]
            copy(piece, piece, b["g_s"].at[first + k - 1], b["g_r"].at[first + k - 1], at(k)).wait_recv()

    def GC():
        load_n.wait()
        load_ng.wait()

        def block(i, carry):
            for k in range(8):
                lanes = pl.ds(pl.multiple_of(i * 1024 + k * 128, 128), 128)
                terms = b["nbuf"][:, lanes].astype(jnp.float32) * b["ngbuf"][:, lanes].astype(jnp.float32)
                b["gain_c"][core, i, k : k + 1, :] = jnp.sum(terms, axis=0, keepdims=True)
            return carry

        lax.fori_loop(0, 8, block, 0)
        mine = b["gain_c"].at[core]
        start(mine, mine, b["g_s"].at[0], b["g_r"].at[0], sibling)

    def GX():
        theirs = b["gain_c"].at[other]
        copy(theirs, theirs, b["g_s"].at[0], b["g_r"].at[0], sibling).wait_recv()
        b["gain_x"][x] = b["gain_c"][0] + b["gain_c"][1]
        for one in peers(at_x, x, 4, b["gain_x"], 1):
            start(*one)

    def GY():
        arrived(x, 4, b["gain_x"], 1, at_x)
        g = b["gain_x"]
        b["gain_y"][y] = (g[0] + g[1]) + (g[2] + g[3])
        for one in peers(at_y, y, 4, b["gain_y"], 4):
            start(*one)

    def GZ():
        arrived(y, 4, b["gain_y"], 4, at_y)
        g = b["gain_y"]
        b["gain_s"][...] = (g[0] + g[1]) + (g[2] + g[3])
        b["gain_z"][z] = b["gain_s"][z]
        for one in peers(at_z, z, 8, b["gain_z"], 7, b["gain_s"]):
            start(*one)

    def GA():
        arrived(z, 8, b["gain_z"], 7, at_z)
        total = b["gain_z"][0]
        for k in range(1, 8):
            total = total + b["gain_z"][k]
        b["gain_a"][z] = total
        for one in peers(at_z, z, 8, b["gain_a"], 14):
            start(*one)

    def GO():
        arrived(z, 8, b["gain_a"], 14, at_z)
        gain_ref[...] = b["gain_a"][...].reshape(64, 128)

    def M(j, o):
        if o == 0:
            copy(*d_copy(j, 0, 0, other)).wait_recv()
            for s in range(1, 5):
                for d in range(2):
                    copy(*d_copy(j, d, s, other)).wait_recv()
        for k in range(2):
            right = b["gbuf"][j, :, :, :, k * 256 : (k + 1) * 256].reshape(2048, 256)
            product = jnp.dot(b["xt"][o], right, preferred_element_type=jnp.float32)
            b["part"][j, o, 2 * k] = product[:, :128]
            b["part"][j, o, 2 * k + 1] = product[:, 128:]
        far = ring(x + 2, 4)
        for d in range(2):
            half = pl.ds(128 * d, 128)
            start(b["part"].at[j, o, far, half], b["xfar"].at[j, o, d], b["u_s"].at[j, o, d], b["u_r"].at[j, o, d], at_x(both[d]))
        for d in range(2):
            start(*near_copy(j, o, d, 1 - d, 2 + d))

    def near_copy(j, o, d, half, slot):
        rows = pl.ds(128 * half, 128)
        return (
            b["part"].at[j, o, ring(x + both[d], 4), rows],
            b["xnear"].at[j, o, d, rows],
            b["u_s"].at[j, o, slot],
            b["u_r"].at[j, o, slot],
            at_x(both[d]),
        )

    def X1(j, o):
        for d in range(2):
            piece = b["xfar"].at[j, o, d]
            copy(piece, piece, b["u_s"].at[j, o, d], b["u_r"].at[j, o, d], at_x(both[d])).wait_recv()
            there = ring(x + both[d], 4)
            rows = pl.ds(128 * d, 128)
            b["part"][j, o, there, rows] = b["part"][j, o, there, rows] + b["xfar"][j, o, d]
            start(*near_copy(j, o, d, d, 4 + d))

    def role(j, o):
        owns = ylo == j % 2
        ahead = lax.rem(ylo + o, 2)
        return owns, ahead

    def y_target(ahead):
        there = ring(y + 1 - 2 * ahead, 4)
        return {YHI: there // 2, YLO: lax.rem(there, 2)}

    def feature(o):
        return lax.rem(yhi + o, 2)

    def y_far(j, o, d):
        rows = pl.ds(128 * d, 128)
        return b["summed"].at[j, o, rows], b["yfar"].at[j, feature(o)], b["y_s"].at[j, o, d], b["yf_r"].at[j, feature(o)], at_y(both[d])

    def y_near(j, o, ahead, late):
        half = ahead if late else 1 - ahead
        rows = pl.ds(pl.multiple_of(128 * half, 128), 128)
        slot = 1 if late else 0
        return (
            b["summed"].at[j, o, rows],
            b["ynear"].at[j, ahead, rows],
            b["y_s"].at[j, o, slot],
            b["yn_r"].at[j, ahead, slot],
            y_target(ahead),
        )

    def X2(j, o):
        for d in range(2):
            for slot, half in ((2 + d, 1 - d), (4 + d, d)):
                piece = b["xnear"].at[j, o, d, pl.ds(128 * half, 128)]
                copy(piece, piece, b["u_s"].at[j, o, slot], b["u_r"].at[j, o, slot], at_x(both[d])).wait_recv()
        b["summed"][j, o] = b["part"][j, o, x] + (b["xnear"][j, o, 0] + b["xnear"][j, o, 1])
        owns, ahead = role(j, o)
        if o == 1:

            @pl.when(owns)
            def _():
                for d in range(2):
                    copy(*y_far(j, o, d)).start()

        @pl.when(jnp.logical_not(owns))
        def _():
            copy(*y_near(j, o, ahead, False)).start()

    def Y1(j, o):
        owns, ahead = role(j, o)

        @pl.when(jnp.logical_not(owns))
        def _():
            piece = b["yfar"].at[j, feature(o)]
            copy(piece, piece, b["y_s"].at[j, o, 1], b["yf_r"].at[j, feature(o)], y_target(ahead)).wait_recv()
            rows = pl.ds(pl.multiple_of(128 * ahead, 128), 128)
            b["summed"][j, o, rows] = b["summed"][j, o, rows] + b["yfar"][j, feature(o)]
            copy(*y_near(j, o, ahead, True)).start()

    def Y2(j):
        owns, _ = role(j, 0)

        @pl.when(owns)
        def _():
            for side in range(2):
                for slot in range(2):
                    half = side if slot else 1 - side
                    piece = b["ynear"].at[j, side, pl.ds(128 * half, 128)]
                    copy(piece, piece, b["y_s"].at[j, 0, 0], b["yn_r"].at[j, side, slot], at_y(1)).wait_recv()
            total = b["summed"][j, 0] + (b["ynear"][j, 0] + b["ynear"][j, 1])
            first = (j // 2) * 128
            out_ref[:, first : first + 128] = total * 0.125

    steps = dict(S=S, E=E, XS=XS, R=R, XO=XO, XA=XA, GC=GC, GX=GX, GY=GY, GZ=GZ, GA=GA, GO=GO, M=M, X1=X1, X2=X2, Y1=Y1, Y2=Y2)
    for name, *which in ORDER:
        steps[name](*which)

    for one in sent:
        one.wait_send()
    for j in range(4):
        for o in range(2):
            owns, ahead = role(j, o)
            if o == 1:

                @pl.when(owns)
                def _():
                    for d in range(2):
                        copy(*y_far(j, o, d)).wait_send()

            @pl.when(jnp.logical_not(owns))
            def _():
                copy(*y_near(j, o, ahead, False)).wait_send()
                copy(*y_near(j, o, ahead, True)).wait_send()


def shards(proj_in, kv_grad, normed, norm_grad, first_moment, second_moment):
    mean_grad, gain = pl.pallas_call(
        exchange,
        out_shape=(jax.ShapeDtypeStruct((256, 256), jnp.float32), jax.ShapeDtypeStruct((64, 128), jnp.float32)),
        in_specs=[pl.BlockSpec(memory_space=pl.ANY)] * 4,
        out_specs=(pl.BlockSpec(memory_space=pltpu.VMEM), pl.BlockSpec(memory_space=pltpu.VMEM)),
        scratch_shapes=list(SCRATCH.values()),
        compiler_params=pltpu.CompilerParams(
            collective_id=0, has_side_effects=True, vmem_limit_bytes=60 * 1024 * 1024
        ),
        name="exchange",
    )(proj_in[0], kv_grad[0], normed[0], norm_grad[0])
    new_first, new_second, update = adam_update(mean_grad, first_moment[0], second_moment[0])
    gain_grad = (gain * 0.125).reshape(1, 8192)
    return (new_first[None], new_second[None], update[None], gain_grad)


def solution(mesh):
    finer = Mesh(mesh.devices.reshape(4, 2, 2, 8, 2), DP_TP)
    return jax.shard_map(
        shards,
        mesh=finer,
        in_specs=(
            P(None, DP, TP),
            P(None, DP_TP, None),
            P(None, DP_TP, None),
            P(None, DP_TP, None),
            P(None, TP, DP),
            P(None, TP, DP),
        ),
        out_specs=(P(None, TP, DP), P(None, TP, DP), P(None, TP, DP), P()),
        check_vma=False,
    )
```

```python
import functools

import jax
import jax.numpy as jnp
from jax import lax
from jax.experimental import pallas as pl
from jax.experimental.pallas import tpu as pltpu
from jax.sharding import Mesh
from jax.sharding import PartitionSpec as P

X, YLO, YHI, Z, CORE = "dp_0", "dp_1", "tp_0", "tp_1", "tp_2"
DP = (X, YLO)
TP = (YHI, Z, CORE)
DP_TP = DP + TP
MESH = pl.DeviceIdType.MESH

beta_one = 0.9
beta_two = 0.95
correct_one = 0.19
correct_two = 0.0975
epsilon = 1e-08

VMEM_LIMIT = 60 * 1024 * 1024

ORDER = (
    ('S', 0), ('XS',), ('S', 1), ('S', 2), ('E', 0, 1), ('E', 1, 1), ('E', 2, 1), ('S', 3), ('E', 1, 2), ('GS',),
    ('R', 0), ('E', 0, 2), ('S', 4), ('E', 2, 2), ('R', 3), ('E', 0, 3), ('E', 1, 3), ('E', 4, 1), ('R', 1),
    ('E', 2, 3), ('E', 3, 1), ('S', 5), ('GX',), ('E', 0, 4), ('E', 1, 4), ('R', 2), ('M', 0, 0), ('M', 1, 0),
    ('E', 4, 2), ('XA', 3), ('E', 2, 4), ('S', 6), ('XA', 0), ('XA', 1), ('M', 2, 0), ('E', 3, 2), ('E', 5, 1),
    ('X1', 0, 0), ('X1', 1, 0), ('XA', 2), ('M', 2, 1), ('M', 0, 1), ('M', 1, 1), ('E', 4, 3), ('S', 7), ('E', 3, 3),
    ('E', 6, 1), ('E', 5, 2), ('X1', 2, 1), ('X1', 0, 1), ('E', 4, 4), ('X1', 2, 0), ('M', 4, 0), ('E', 3, 4),
    ('M', 4, 1), ('E', 7, 1), ('GY',), ('E', 6, 2), ('M', 3, 0), ('X2', 2, 1), ('M', 3, 1), ('E', 5, 3), ('X1', 4, 1),
    ('X1', 4, 0), ('E', 7, 2), ('X1', 1, 1), ('E', 6, 3), ('E', 5, 4), ('X1', 3, 0), ('X1', 3, 1), ('GZ',),
    ('X2', 0, 0), ('E', 7, 3), ('M', 5, 0), ('X2', 1, 0), ('E', 6, 4), ('X2', 0, 1), ('M', 5, 1), ('X2', 4, 0),
    ('X2', 3, 0), ('X2', 4, 1), ('M', 6, 0), ('E', 7, 4), ('X2', 3, 1), ('M', 7, 0), ('X2', 2, 0), ('M', 7, 1),
    ('X2', 1, 1), ('Y1', 4, 1), ('M', 6, 1), ('Y1', 0, 1), ('Y1', 1, 0), ('Y1', 3, 1), ('X1', 5, 1), ('Y1', 1, 1),
    ('Y1', 4, 0), ('X1', 7, 1), ('X1', 6, 1), ('Y1', 2, 0), ('Y1', 2, 1), ('Y1', 0, 0), ('X1', 5, 0), ('Y1', 3, 0),
    ('X1', 7, 0), ('X2', 5, 1), ('GA',), ('X2', 7, 1), ('X1', 6, 0), ('X2', 6, 1), ('X2', 5, 0), ('X2', 7, 0),
    ('Y1', 7, 0), ('Y2', 1), ('Y2', 3), ('Y1', 5, 0), ('X2', 6, 0), ('Y1', 6, 1), ('Y1', 6, 0), ('Y1', 5, 1),
    ('Y2', 4), ('Y2', 5), ('Y2', 0), ('Y2', 2), ('Y1', 7, 1), ('GO',), ('Y2', 7), ('Y2', 6),
)


SCRATCH = dict(
    raw=pltpu.VMEM((128, 2048), jnp.bfloat16),
    gbuf=pltpu.VMEM((8, 8, 2, 128, 256), jnp.bfloat16),
    xown=pltpu.VMEM((2048, 256), jnp.bfloat16),
    xoth=pltpu.VMEM((2, 4, 256, 256), jnp.bfloat16),
    relay=pltpu.VMEM((2, 4, 256, 256), jnp.bfloat16),
    xt=pltpu.VMEM((2, 256, 2048), jnp.bfloat16),
    part=pltpu.VMEM((8, 2, 4, 128, 128), jnp.float32),
    xfar=pltpu.VMEM((8, 2, 2, 64, 128), jnp.float32),
    xnear=pltpu.VMEM((8, 2, 2, 128, 128), jnp.float32),
    summed=pltpu.VMEM((8, 2, 128, 128), jnp.float32),
    yfar=pltpu.VMEM((8, 2, 64, 128), jnp.float32),
    ynear=pltpu.VMEM((8, 2, 128, 128), jnp.float32),
    nbuf=pltpu.VMEM((128, 8192), jnp.bfloat16),
    ngbuf=pltpu.VMEM((128, 8192), jnp.bfloat16),
    gain_c=pltpu.VMEM((2, 8, 8, 128), jnp.float32),
    gain_x=pltpu.VMEM((4, 8, 8, 128), jnp.float32),
    gain_y=pltpu.VMEM((4, 8, 8, 128), jnp.float32),
    gain_s=pltpu.VMEM((8, 8, 128), jnp.float32),
    gain_z=pltpu.VMEM((8, 8, 128), jnp.float32),
    gain_a=pltpu.VMEM((8, 8, 128), jnp.float32),
    load=pltpu.SemaphoreType.DMA((4,)),
    z_s=pltpu.SemaphoreType.DMA((8,)),
    z_r=pltpu.SemaphoreType.DMA((8, 4)),
    d_s=pltpu.SemaphoreType.DMA((8,)),
    d_r=pltpu.SemaphoreType.DMA((8,)),
    x1_s=pltpu.SemaphoreType.DMA,
    x1_r=pltpu.SemaphoreType.DMA((4,)),
    x2_s=pltpu.SemaphoreType.DMA,
    x2_r=pltpu.SemaphoreType.DMA((4,)),
    u_s=pltpu.SemaphoreType.DMA((8, 2)),
    far_r=pltpu.SemaphoreType.DMA((8, 2)),
    near_r=pltpu.SemaphoreType.DMA((8, 2)),
    y_s=pltpu.SemaphoreType.DMA((8, 2)),
    yf_r=pltpu.SemaphoreType.DMA((8, 2)),
    yn_r=pltpu.SemaphoreType.DMA((8,)),
    g_s=pltpu.SemaphoreType.DMA((5,)),
    g_r=pltpu.SemaphoreType.DMA((5,)),
)


def exchange(x_hbm, g_hbm, n_hbm, ng_hbm, out_ref, gain_ref, *scratch):
    b = dict(zip(SCRATCH, scratch, strict=True))
    x, ylo, yhi = lax.axis_index(X), lax.axis_index(YLO), lax.axis_index(YHI)
    z, core = lax.axis_index(Z), lax.axis_index(CORE)
    y = yhi * 2 + ylo
    other = 1 - core

    def ring(value, size):
        return lax.rem(value + size, size)

    def at_x(step):
        return {X: ring(x + step, 4)}

    def at_y(step):
        there = ring(y + step, 4)
        return {YHI: there // 2, YLO: lax.rem(there, 2)}

    def at_z(step):
        return {Z: ring(z + step, 8)}

    sibling = {CORE: other}
    both = (1, -1)

    def copy(src, dst, send, recv, to):
        return pltpu.make_async_remote_copy(
            src_ref=src, dst_ref=dst, send_sem=send, recv_sem=recv, device_id=to, device_id_type=MESH
        )

    def start(*args):
        copy(*args).start()

    def landed(ref, sem):
        pltpu.make_async_copy(ref, ref, sem).wait()

    own_rows = pl.multiple_of(yhi * 2048, 2048)
    away_rows = pl.multiple_of((1 - yhi) * 2048, 2048)
    load_g = pltpu.make_async_copy(g_hbm, b["raw"], b["load"].at[0])
    load_x = pltpu.make_async_copy(x_hbm.at[pl.ds(own_rows, 2048), :], b["xown"], b["load"].at[1])
    load_n = pltpu.make_async_copy(n_hbm, b["nbuf"], b["load"].at[2])
    load_ng = pltpu.make_async_copy(ng_hbm, b["ngbuf"], b["load"].at[3])
    for one in (load_g, load_x, load_n, load_ng):
        one.start()

    barrier = pltpu.get_barrier_semaphore()
    greeted = [sibling, at_z(1), at_z(-1)] + [at_y(k) for k in range(1, 4)] + [at_x(k) for k in range(1, 4)]
    for peer in greeted:
        pl.semaphore_signal(barrier, inc=1, device_id=peer, device_id_type=MESH)

    load_g.wait()
    for low in range(2):
        for pair in range(2):
            blocks = []
            for k in range(4):
                first = k * 512 + low * 256 + pair * 128
                blocks.append(b["raw"][:, first : first + 128])
            for side in range(2):
                lanes = slice(64 * side, 64 * side + 64)
                j = (pair * 2 + side) * 2 + low
                b["gbuf"][j, z, core] = jnp.concatenate([block[:, lanes] for block in blocks], axis=1)
    load_x.wait()
    for k in range(8):
        b["xt"][0, :, k * 256 : (k + 1) * 256] = b["xown"][k * 256 : (k + 1) * 256, :].T
    load_n.wait()
    load_ng.wait()

    def block_sum(i, carry):
        for k in range(8):
            lanes = pl.ds(pl.multiple_of(i * 1024 + k * 128, 128), 128)
            terms = b["nbuf"][:, lanes].astype(jnp.float32) * b["ngbuf"][:, lanes].astype(jnp.float32)
            b["gain_c"][core, i, k : k + 1, :] = jnp.sum(terms, axis=0, keepdims=True)
        return carry

    lax.fori_loop(0, 8, block_sum, 0)
    pl.semaphore_wait(barrier, len(greeted))

    def z_send(j, d, s):
        piece = b["gbuf"].at[j, ring(z - (s - 1) * both[d], 8), core]
        if s == 4:
            piece = piece.at[pl.ds(64 * d, 64)]
        start(piece, piece, b["z_s"].at[j], b["z_r"].at[j, s - 1], at_z(both[d]))

    def d_send(j, d, s):
        piece = b["gbuf"].at[j, ring(z - s * both[d], 8), core]
        if s == 4:
            piece = piece.at[pl.ds(64 * d, 64)]
        start(piece, piece, b["d_s"].at[j], b["d_r"].at[j], sibling)

    def S(j):
        for d in range(2):
            z_send(j, d, 1)
        d_send(j, 0, 0)

    def E(j, s):
        landed(b["gbuf"].at[j, pl.ds(0, 2 if s < 4 else 1), core], b["z_r"].at[j, s - 1])
        for d in range(2):
            if s < 4:
                z_send(j, d, s + 1)
            d_send(j, d, s)

    def relay_copy(d, m):
        rows = pl.multiple_of(away_rows + d * 1024 + m * 256, 256)
        return x_hbm.at[pl.ds(rows, 256), :], b["relay"].at[d, m], b["x1_s"], b["x1_r"].at[m], at_y(both[d])

    def onward_copy(d, m):
        return b["relay"].at[d, m], b["xoth"].at[d, m], b["x2_s"], b["x2_r"].at[m], at_y(both[d])

    def XS():
        for m in range(4):
            for d in range(2):
                start(*relay_copy(d, m))

    def R(m):
        landed(b["relay"].at[:, m], b["x1_r"].at[m])
        for d in range(2):
            start(*onward_copy(d, m))

    def XA(m):
        landed(b["xoth"].at[:, m], b["x2_r"].at[m])
        for d in range(2):
            k = d * 4 + m
            b["xt"][1, :, k * 256 : (k + 1) * 256] = b["xoth"][d, m].T

    def spread(at, me, count, buf, sem, source=None):
        for k in range(1, count):
            src = buf.at[me] if source is None else source.at[ring(me + k, count)]
            start(src, buf.at[me], b["g_s"].at[sem], b["g_r"].at[sem], at(k))

    def arrived(count, buf, sem):
        landed(buf.at[pl.ds(0, count - 1)], b["g_r"].at[sem])

    def GS():
        mine = b["gain_c"].at[core]
        start(mine, mine, b["g_s"].at[0], b["g_r"].at[0], sibling)

    def GX():
        landed(b["gain_c"].at[0], b["g_r"].at[0])
        b["gain_x"][x] = b["gain_c"][0] + b["gain_c"][1]
        spread(at_x, x, 4, b["gain_x"], 1)

    def GY():
        arrived(4, b["gain_x"], 1)
        g = b["gain_x"]
        b["gain_y"][y] = (g[0] + g[1]) + (g[2] + g[3])
        spread(at_y, y, 4, b["gain_y"], 2)

    def GZ():
        arrived(4, b["gain_y"], 2)
        g = b["gain_y"]
        b["gain_s"][...] = (g[0] + g[1]) + (g[2] + g[3])
        b["gain_z"][z] = b["gain_s"][z]
        spread(at_z, z, 8, b["gain_z"], 3, b["gain_s"])

    def GA():
        arrived(8, b["gain_z"], 3)
        total = b["gain_z"][0]
        for k in range(1, 8):
            total = total + b["gain_z"][k]
        b["gain_a"][z] = total
        spread(at_z, z, 8, b["gain_a"], 4)

    def GO():
        arrived(8, b["gain_a"], 4)
        gain_ref[...] = b["gain_a"][...]

    def M(j, o):
        if o == 0:
            landed(b["gbuf"].at[j, :, other], b["d_r"].at[j])
        low = lax.broadcasted_iota(jnp.int32, (128, 128), 1) < 64
        packed = []
        for h in range(2):
            product = jnp.dot(
                b["xt"][o, :, h * 1024 : (h + 1) * 1024],
                b["gbuf"][j, 4 * h : 4 * h + 4].reshape(1024, 256),
                preferred_element_type=jnp.float32,
            )
            for k in range(2):
                lanes = slice(128 * k, 128 * k + 128)
                upper, lower = product[:128, lanes], product[128:, lanes]
                packed.append(jnp.where(low, upper, pltpu.roll(lower, 64, 1)))
                packed.append(jnp.where(low, pltpu.roll(upper, 64, 1), lower))
        for k in range(4):
            b["part"][j, o, k] = packed[k] + packed[4 + k]
        far = ring(x + 2, 4)
        for d in range(2):
            half = pl.ds(64 * d, 64)
            start(b["part"].at[j, o, far, half], b["xfar"].at[j, o, d], b["u_s"].at[j, o], b["far_r"].at[j, o], at_x(both[d]))
        for d in range(2):
            near_send(j, o, d, 1 - d)

    def near_send(j, o, d, half):
        rows = pl.ds(64 * half, 64)
        start(
            b["part"].at[j, o, ring(x + both[d], 4), rows],
            b["xnear"].at[j, o, d, rows],
            b["u_s"].at[j, o],
            b["near_r"].at[j, o],
            at_x(both[d]),
        )

    def X1(j, o):
        landed(b["xfar"].at[j, o], b["far_r"].at[j, o])
        for d in range(2):
            there = ring(x + both[d], 4)
            rows = pl.ds(64 * d, 64)
            b["part"][j, o, there, rows] = b["part"][j, o, there, rows] + b["xfar"][j, o, d]
            near_send(j, o, d, d)

    def role(j, o):
        owns = ylo == j % 2
        ahead = lax.rem(ylo + o, 2)
        return owns, ahead

    def y_target(ahead):
        there = ring(y + 1 - 2 * ahead, 4)
        return {YHI: there // 2, YLO: lax.rem(there, 2)}

    def feature(o):
        return lax.rem(yhi + o, 2)

    def y_far(j, o, d):
        rows = pl.ds(64 * d, 64)
        return b["summed"].at[j, o, rows], b["yfar"].at[j, feature(o)], b["y_s"].at[j, o], b["yf_r"].at[j, feature(o)], at_y(both[d])

    def y_near(j, o, ahead, late):
        half = ahead if late else 1 - ahead
        rows = pl.ds(pl.multiple_of(64 * half, 64), 64)
        return (
            b["summed"].at[j, o, rows],
            b["ynear"].at[j, ahead, rows],
            b["y_s"].at[j, o],
            b["yn_r"].at[j],
            y_target(ahead),
        )

    def X2(j, o):
        landed(b["xnear"].at[j, o], b["near_r"].at[j, o])
        b["summed"][j, o] = b["part"][j, o, x] + (b["xnear"][j, o, 0] + b["xnear"][j, o, 1])
        owns, ahead = role(j, o)
        if o == 1:

            @pl.when(owns)
            def _():
                for d in range(2):
                    copy(*y_far(j, o, d)).start()

        @pl.when(jnp.logical_not(owns))
        def _():
            copy(*y_near(j, o, ahead, False)).start()

    def Y1(j, o):
        owns, ahead = role(j, o)

        @pl.when(jnp.logical_not(owns))
        def _():
            landed(b["yfar"].at[j, feature(o)], b["yf_r"].at[j, feature(o)])
            rows = pl.ds(pl.multiple_of(64 * ahead, 64), 64)
            b["summed"][j, o, rows] = b["summed"][j, o, rows] + b["yfar"][j, feature(o)]
            copy(*y_near(j, o, ahead, True)).start()

    def Y2(j):
        owns, _ = role(j, 0)

        @pl.when(owns)
        def _():
            landed(b["ynear"].at[j], b["yn_r"].at[j])
            total = b["summed"][j, 0] + (b["ynear"][j, 0] + b["ynear"][j, 1])
            total = total * 0.125
            lanes = slice((j // 2) * 64, (j // 2) * 64 + 64)
            out_ref[:128, lanes] = total[:, :64]
            out_ref[128:, lanes] = total[:, 64:]

    steps = dict(S=S, E=E, XS=XS, R=R, XA=XA, GS=GS, GX=GX, GY=GY, GZ=GZ, GA=GA, GO=GO, M=M, X1=X1, X2=X2, Y1=Y1, Y2=Y2)
    for name, *which in ORDER:
        steps[name](*which)

    landed(x_hbm.at[pl.ds(0, 2048), :], b["x1_s"])
    landed(b["xoth"], b["x2_s"])
    for sem, piece in enumerate((b["gain_c"].at[0], b["gain_x"].at[pl.ds(0, 3)], b["gain_y"].at[pl.ds(0, 3)])):
        landed(piece, b["g_s"].at[sem])
    for sem in (3, 4):
        landed(b["gain_a"].at[pl.ds(0, 7)], b["g_s"].at[sem])
    for j in range(8):
        landed(b["gbuf"].at[j, pl.ds(0, 7), 0], b["z_s"].at[j])
        landed(b["gbuf"].at[j, :, 0], b["d_s"].at[j])
        for o in range(2):
            landed(b["part"].at[j, o, pl.ds(0, 3)], b["u_s"].at[j, o])
            owns, _ = role(j, o)
            if o == 1:
                landed(b["summed"].at[j, o], b["y_s"].at[j, o])
            else:

                @pl.when(jnp.logical_not(owns))
                def _():
                    landed(b["summed"].at[j, o], b["y_s"].at[j, o])


def finish(grad_ref, gain_ref, first_ref, second_ref, new_first_ref, new_second_ref, update_ref, gain_grad_ref):
    grad = grad_ref[...]
    new_first = beta_one * first_ref[...] + (1.0 - beta_one) * grad
    new_second = beta_two * second_ref[...] + (1.0 - beta_two) * grad * grad
    new_first_ref[...] = new_first
    new_second_ref[...] = new_second
    update_ref[...] = new_first / correct_one / (jnp.sqrt(new_second / correct_two) + epsilon)
    for i in range(8):
        for k in range(8):
            first = (i * 8 + k) * 128
            gain_grad_ref[0:1, first : first + 128] = gain_ref[i, k : k + 1, :] * 0.125


def shards(proj_in, kv_grad, normed, norm_grad, first_moment, second_moment):
    vmem = pl.BlockSpec(memory_space=pltpu.VMEM)
    mean_grad, gain = pl.pallas_call(
        exchange,
        out_shape=(jax.ShapeDtypeStruct((256, 256), jnp.float32), jax.ShapeDtypeStruct((8, 8, 128), jnp.float32)),
        in_specs=[pl.BlockSpec(memory_space=pltpu.HBM)] * 4,
        out_specs=(vmem, vmem),
        scratch_shapes=list(SCRATCH.values()),
        compiler_params=pltpu.CompilerParams(
            collective_id=0, has_side_effects=True, vmem_limit_bytes=VMEM_LIMIT
        ),
        name="exchange",
    )(proj_in[0], kv_grad[0], normed[0], norm_grad[0])
    block = jax.ShapeDtypeStruct((256, 256), jnp.float32)
    new_first, new_second, update, gain_grad = pl.pallas_call(
        finish,
        out_shape=(block, block, block, jax.ShapeDtypeStruct((1, 8192), jnp.float32)),
        in_specs=[vmem] * 4,
        out_specs=(vmem,) * 4,
        name="finish",
    )(mean_grad, gain, first_moment[0], second_moment[0])
    return (new_first[None], new_second[None], update[None], gain_grad)


def solution(mesh):
    finer = Mesh(mesh.devices.reshape(4, 2, 2, 8, 2), DP_TP)
    return jax.shard_map(
        shards,
        mesh=finer,
        in_specs=(
            P(None, DP, TP),
            P(None, DP_TP, None),
            P(None, DP_TP, None),
            P(None, DP_TP, None),
            P(None, TP, DP),
            P(None, TP, DP),
        ),
        out_specs=(P(None, TP, DP), P(None, TP, DP), P(None, TP, DP), P()),
        check_vma=False,
    )
```

```python
import functools

import jax
import jax.numpy as jnp
from jax import lax
from jax.experimental import pallas as pl
from jax.experimental.pallas import tpu as pltpu
from jax.sharding import Mesh
from jax.sharding import PartitionSpec as P

X, YLO, YHI, Z, CORE = "dp_0", "dp_1", "tp_0", "tp_1", "tp_2"
DP = (X, YLO)
TP = (YHI, Z, CORE)
DP_TP = DP + TP
MESH = pl.DeviceIdType.MESH

beta_one = 0.9
beta_two = 0.95
correct_one = 0.19
correct_two = 0.0975
epsilon = 1e-08

VMEM_LIMIT = 60 * 1024 * 1024

YFIRST = (6,)
ORDER = (
    ('S', 0), ('S', 1), ('XS',), ('S', 2), ('E', 0, 1), ('XO',), ('E', 1, 1), ('S', 3), ('E', 0, 2), ('GC',),
    ('E', 2, 1), ('E', 1, 2), ('GS',), ('R', 0), ('E', 0, 3), ('R', 2), ('S', 4), ('E', 2, 2), ('R', 3), ('E', 1, 3),
    ('S', 5), ('E', 3, 1), ('E', 0, 4), ('XA', 0), ('E', 2, 3), ('R', 1), ('XA', 2), ('E', 1, 4), ('E', 4, 1),
    ('M', 0, 0), ('S', 6), ('GX',), ('M', 1, 0), ('I', 0, 0), ('I', 1, 0), ('E', 3, 2), ('E', 2, 4), ('X1', 0, 0),
    ('E', 4, 2), ('S', 7), ('M', 2, 0), ('XA', 3), ('XA', 1), ('M', 1, 1), ('E', 6, 1), ('GY',), ('I', 1, 1),
    ('M', 2, 1), ('M', 0, 1), ('X1', 1, 0), ('I', 2, 1), ('X2', 0, 0), ('E', 4, 3), ('E', 3, 3), ('X1', 2, 1),
    ('X1', 1, 1), ('I', 0, 1), ('E', 5, 1), ('E', 6, 2), ('E', 4, 4), ('X1', 0, 1), ('I', 2, 0), ('X1', 2, 0),
    ('E', 7, 1), ('E', 3, 4), ('M', 3, 0), ('E', 5, 2), ('M', 3, 1), ('M', 4, 0), ('X2', 2, 1), ('I', 4, 0),
    ('E', 6, 3), ('E', 7, 2), ('I', 3, 0), ('X2', 1, 0), ('X2', 2, 0), ('M', 4, 1), ('X1', 3, 1), ('E', 5, 3),
    ('I', 4, 1), ('E', 6, 4), ('X1', 3, 0), ('I', 3, 1), ('E', 7, 3), ('X1', 4, 0), ('X2', 1, 1), ('M', 6, 0),
    ('E', 5, 4), ('M', 6, 1), ('X1', 4, 1), ('M', 5, 0), ('E', 7, 4), ('GZ',), ('X2', 3, 1), ('I', 5, 0), ('M', 5, 1),
    ('X2', 0, 1), ('M', 7, 0), ('M', 7, 1), ('Y1', 2, 1), ('X2', 3, 0), ('I', 5, 1), ('Y1', 2, 0), ('Y1', 6, 1),
    ('Y1', 6, 0), ('X2', 4, 1), ('X1', 5, 1), ('I', 7, 1), ('X1', 7, 1), ('Y1', 3, 1), ('X1', 5, 0), ('Y1', 0, 0),
    ('GA',), ('Y1', 1, 1), ('I', 7, 0), ('X1', 7, 0), ('X2', 4, 0), ('X2', 5, 1), ('Y1', 3, 0), ('Y1', 1, 0),
    ('Y1', 0, 1), ('X0', 6), ('X2', 7, 1), ('Y1', 4, 0), ('X2', 5, 0), ('Y1', 5, 0), ('Y2', 2), ('Y1', 5, 1),
    ('Y2', 3), ('GO',), ('X2', 7, 0), ('Y2', 0), ('Y1', 4, 1), ('Y1', 7, 1), ('Y1', 7, 0), ('X1', 6, 0), ('Y2', 4),
    ('Y2', 5), ('Y2', 1), ('Y2', 7), ('X2', 6, 0),
)


SCRATCH = dict(
    raw=pltpu.VMEM((128, 2048), jnp.bfloat16),
    gbuf=pltpu.VMEM((8, 8, 2, 128, 256), jnp.bfloat16),
    xown=pltpu.VMEM((2048, 256), jnp.bfloat16),
    xoth=pltpu.VMEM((2, 4, 256, 256), jnp.bfloat16),
    relay=pltpu.VMEM((2, 4, 256, 256), jnp.bfloat16),
    xt=pltpu.VMEM((2, 256, 2048), jnp.bfloat16),
    part=pltpu.VMEM((8, 2, 4, 128, 128), jnp.float32),
    xfar=pltpu.VMEM((8, 2, 2, 64, 128), jnp.float32),
    xnear=pltpu.VMEM((8, 2, 2, 128, 128), jnp.float32),
    summed=pltpu.VMEM((8, 2, 128, 128), jnp.float32),
    yfar=pltpu.VMEM((8, 2, 64, 128), jnp.float32),
    ynear=pltpu.VMEM((8, 2, 128, 128), jnp.float32),
    yfar4=pltpu.VMEM((max(1, len(YFIRST)), 2, 4, 64, 128), jnp.float32),
    ynear4=pltpu.VMEM((max(1, len(YFIRST)), 2, 4, 128, 128), jnp.float32),
    nbuf=pltpu.VMEM((128, 8192), jnp.bfloat16),
    ngbuf=pltpu.VMEM((128, 8192), jnp.bfloat16),
    gain_c=pltpu.VMEM((2, 8, 8, 128), jnp.float32),
    gain_x=pltpu.VMEM((4, 8, 8, 128), jnp.float32),
    gain_y=pltpu.VMEM((4, 8, 8, 128), jnp.float32),
    gain_s=pltpu.VMEM((8, 8, 128), jnp.float32),
    gain_z=pltpu.VMEM((8, 8, 128), jnp.float32),
    gain_a=pltpu.VMEM((8, 8, 128), jnp.float32),
    load=pltpu.SemaphoreType.DMA((4,)),
    z_s=pltpu.SemaphoreType.DMA((8,)),
    z_r=pltpu.SemaphoreType.DMA((8, 4, 2)),
    d_s=pltpu.SemaphoreType.DMA((8,)),
    d_r=pltpu.SemaphoreType.DMA((8,)),
    x1_s=pltpu.SemaphoreType.DMA,
    x1_r=pltpu.SemaphoreType.DMA((2, 4)),
    x2_s=pltpu.SemaphoreType.DMA,
    x2_r=pltpu.SemaphoreType.DMA((4,)),
    u_s=pltpu.SemaphoreType.DMA((8, 2)),
    far_r=pltpu.SemaphoreType.DMA((8, 2)),
    near_r=pltpu.SemaphoreType.DMA((8, 2)),
    y_s=pltpu.SemaphoreType.DMA((8, 2)),
    yf_r=pltpu.SemaphoreType.DMA((8, 2)),
    yn_r=pltpu.SemaphoreType.DMA((8,)),
    g_s=pltpu.SemaphoreType.DMA((5,)),
    g_r=pltpu.SemaphoreType.DMA((5,)),
)


def exchange(x_hbm, g_hbm, n_hbm, ng_hbm, out_ref, gain_ref, *scratch):
    b = dict(zip(SCRATCH, scratch, strict=True))
    x, ylo, yhi = lax.axis_index(X), lax.axis_index(YLO), lax.axis_index(YHI)
    z, core = lax.axis_index(Z), lax.axis_index(CORE)
    y = yhi * 2 + ylo
    other = 1 - core

    def ring(value, size):
        return lax.rem(value + size, size)

    def at_x(step):
        return {X: ring(x + step, 4)}

    def at_y(step):
        there = ring(y + step, 4)
        return {YHI: there // 2, YLO: lax.rem(there, 2)}

    def at_z(step):
        return {Z: ring(z + step, 8)}

    sibling = {CORE: other}
    both = (1, -1)

    def copy(src, dst, send, recv, to):
        return pltpu.make_async_remote_copy(
            src_ref=src, dst_ref=dst, send_sem=send, recv_sem=recv, device_id=to, device_id_type=MESH
        )

    def start(*args):
        copy(*args).start()

    def landed(ref, sem):
        pltpu.make_async_copy(ref, ref, sem).wait()

    own_rows = pl.multiple_of(yhi * 2048, 2048)
    away_rows = pl.multiple_of((1 - yhi) * 2048, 2048)
    load_g = pltpu.make_async_copy(g_hbm, b["raw"], b["load"].at[0])
    load_x = pltpu.make_async_copy(x_hbm.at[pl.ds(own_rows, 2048), :], b["xown"], b["load"].at[1])
    load_n = pltpu.make_async_copy(n_hbm, b["nbuf"], b["load"].at[2])
    load_ng = pltpu.make_async_copy(ng_hbm, b["ngbuf"], b["load"].at[3])
    for one in (load_g, load_x, load_n, load_ng):
        one.start()

    barrier = pltpu.get_barrier_semaphore()
    greeted = [sibling, at_z(1), at_z(-1)] + [at_y(k) for k in range(1, 4)] + [at_x(k) for k in range(1, 4)]
    for peer in greeted:
        pl.semaphore_signal(barrier, inc=1, device_id=peer, device_id_type=MESH)

    load_g.wait()
    for low in range(2):
        for pair in range(2):
            blocks = []
            for k in range(4):
                first = k * 512 + low * 256 + pair * 128
                blocks.append(b["raw"][:, first : first + 128])
            for side in range(2):
                lanes = slice(64 * side, 64 * side + 64)
                j = (pair * 2 + side) * 2 + low
                b["gbuf"][j, z, core] = jnp.concatenate([block[:, lanes] for block in blocks], axis=1)
    pl.semaphore_wait(barrier, len(greeted))

    def z_send(j, d, s):
        piece = b["gbuf"].at[j, ring(z - (s - 1) * both[d], 8), core]
        if s == 4:
            piece = piece.at[pl.ds(64 * d, 64)]
        start(piece, piece, b["z_s"].at[j], b["z_r"].at[j, s - 1, d], at_z(both[d]))

    def d_send(j, d, s):
        piece = b["gbuf"].at[j, ring(z - s * both[d], 8), core]
        if s == 4:
            piece = piece.at[pl.ds(64 * d, 64)]
        start(piece, piece, b["d_s"].at[j], b["d_r"].at[j], sibling)

    def XO():
        load_x.wait()
        for k in range(8):
            b["xt"][0, :, k * 256 : (k + 1) * 256] = b["xown"][k * 256 : (k + 1) * 256, :].T

    def S(j):
        for d in range(2):
            z_send(j, d, 1)
        d_send(j, 0, 0)

    def E(j, s):
        for d in range(2):
            piece = b["gbuf"].at[j, 0, core]
            landed(piece if s < 4 else piece.at[pl.ds(0, 64)], b["z_r"].at[j, s - 1, d])
            if s < 4:
                z_send(j, d, s + 1)
            d_send(j, d, s)

    def relay_copy(d, m):
        rows = pl.multiple_of(away_rows + d * 1024 + m * 256, 256)
        return x_hbm.at[pl.ds(rows, 256), :], b["relay"].at[d, m], b["x1_s"], b["x1_r"].at[d, m], at_y(both[d])

    def onward_copy(d, m):
        return b["relay"].at[d, m], b["xoth"].at[d, m], b["x2_s"], b["x2_r"].at[m], at_y(both[d])

    def XS():
        for m in range(4):
            for d in range(2):
                start(*relay_copy(d, m))

    def R(m):
        for d in range(2):
            landed(b["relay"].at[d, m], b["x1_r"].at[d, m])
            start(*onward_copy(d, m))

    def XA(m):
        landed(b["xoth"].at[:, m], b["x2_r"].at[m])
        for d in range(2):
            k = d * 4 + m
            b["xt"][1, :, k * 256 : (k + 1) * 256] = b["xoth"][d, m].T

    def spread(at, me, count, buf, sem, source=None):
        for k in range(1, count):
            src = buf.at[me] if source is None else source.at[ring(me + k, count)]
            start(src, buf.at[me], b["g_s"].at[sem], b["g_r"].at[sem], at(k))

    def arrived(count, buf, sem):
        landed(buf.at[pl.ds(0, count - 1)], b["g_r"].at[sem])

    def GC():
        load_n.wait()
        load_ng.wait()

        def block_sum(i, carry):
            for k in range(8):
                lanes = pl.ds(pl.multiple_of(i * 1024 + k * 128, 128), 128)
                terms = b["nbuf"][:, lanes].astype(jnp.float32) * b["ngbuf"][:, lanes].astype(jnp.float32)
                b["gain_c"][core, i, k : k + 1, :] = jnp.sum(terms, axis=0, keepdims=True)
            return carry

        lax.fori_loop(0, 8, block_sum, 0)

    def GS():
        mine = b["gain_c"].at[core]
        start(mine, mine, b["g_s"].at[0], b["g_r"].at[0], sibling)

    def GX():
        landed(b["gain_c"].at[0], b["g_r"].at[0])
        b["gain_x"][x] = b["gain_c"][0] + b["gain_c"][1]
        spread(at_x, x, 4, b["gain_x"], 1)

    def GY():
        arrived(4, b["gain_x"], 1)
        g = b["gain_x"]
        b["gain_y"][y] = (g[0] + g[1]) + (g[2] + g[3])
        spread(at_y, y, 4, b["gain_y"], 2)

    def GZ():
        arrived(4, b["gain_y"], 2)
        g = b["gain_y"]
        b["gain_s"][...] = (g[0] + g[1]) + (g[2] + g[3])
        b["gain_z"][z] = b["gain_s"][z]
        spread(at_z, z, 8, b["gain_z"], 3, b["gain_s"])

    def GA():
        arrived(8, b["gain_z"], 3)
        total = b["gain_z"][0]
        for k in range(1, 8):
            total = total + b["gain_z"][k]
        b["gain_a"][z] = total
        spread(at_z, z, 8, b["gain_a"], 4)

    def GO():
        arrived(8, b["gain_a"], 4)
        gain_ref[...] = b["gain_a"][...]

    def M(j, o):
        if o == 0:
            landed(b["gbuf"].at[j, :, other], b["d_r"].at[j])
        low = lax.broadcasted_iota(jnp.int32, (128, 128), 1) < 64
        packed = []
        for h in range(2):
            product = jnp.dot(
                b["xt"][o, :, h * 1024 : (h + 1) * 1024],
                b["gbuf"][j, 4 * h : 4 * h + 4].reshape(1024, 256),
                preferred_element_type=jnp.float32,
            )
            for k in range(2):
                lanes = slice(128 * k, 128 * k + 128)
                upper, lower = product[:128, lanes], product[128:, lanes]
                packed.append(jnp.where(low, upper, pltpu.roll(lower, 64, 1)))
                packed.append(jnp.where(low, pltpu.roll(upper, 64, 1), lower))
        for k in range(4):
            b["part"][j, o, k] = packed[k] + packed[4 + k]
        if j in YFIRST:
            y_first_sends(j, o)
        else:
            far_sends(j, o)

    def far_sends(j, o):
        for d in range(2):
            half = pl.ds(64 * d, 64)
            start(
                b["part"].at[j, o, ring(x + 2, 4), half],
                b["xfar"].at[j, o, d],
                b["u_s"].at[j, o],
                b["far_r"].at[j, o],
                at_x(both[d]),
            )

    def I(j, o):
        for d in range(2):
            near_send(j, o, d, 1 - d)

    def near_send(j, o, d, half):
        rows = pl.ds(64 * half, 64)
        start(
            b["part"].at[j, o, ring(x + both[d], 4), rows],
            b["xnear"].at[j, o, d, rows],
            b["u_s"].at[j, o],
            b["near_r"].at[j, o],
            at_x(both[d]),
        )

    def where_owned(j):
        return pl.when(ylo == j % 2) if j in YFIRST else lambda step: step()

    def X1(j, o):
        @where_owned(j)
        def _():
            landed(b["xfar"].at[j, o], b["far_r"].at[j, o])
            for d in range(2):
                there = ring(x + both[d], 4)
                rows = pl.ds(64 * d, 64)
                b["part"][j, o, there, rows] = b["part"][j, o, there, rows] + b["xfar"][j, o, d]
                near_send(j, o, d, d)

    def role(j, o):
        owns = ylo == j % 2
        ahead = lax.rem(ylo + o, 2)
        return owns, ahead

    def y_target(ahead):
        there = ring(y + 1 - 2 * ahead, 4)
        return {YHI: there // 2, YLO: lax.rem(there, 2)}

    def feature(o):
        return lax.rem(yhi + o, 2)

    def y_far(j, o, d):
        rows = pl.ds(64 * d, 64)
        return b["summed"].at[j, o, rows], b["yfar"].at[j, feature(o)], b["y_s"].at[j, o], b["yf_r"].at[j, feature(o)], at_y(both[d])

    def y_near(j, o, ahead, late):
        half = ahead if late else 1 - ahead
        rows = pl.ds(pl.multiple_of(64 * half, 64), 64)
        return (
            b["summed"].at[j, o, rows],
            b["ynear"].at[j, ahead, rows],
            b["y_s"].at[j, o],
            b["yn_r"].at[j],
            y_target(ahead),
        )

    def put(j, total):
        total = total * 0.125
        lanes = slice((j // 2) * 64, (j // 2) * 64 + 64)
        out_ref[:128, lanes] = total[:, :64]
        out_ref[128:, lanes] = total[:, 64:]

    def X2(j, o):
        if j in YFIRST:

            @where_owned(j)
            def _():
                landed(b["xnear"].at[j, o], b["near_r"].at[j, o])
                put(j, b["part"][j, o, x] + (b["xnear"][j, o, 0] + b["xnear"][j, o, 1]))

            return
        landed(b["xnear"].at[j, o], b["near_r"].at[j, o])
        b["summed"][j, o] = b["part"][j, o, x] + (b["xnear"][j, o, 0] + b["xnear"][j, o, 1])
        owns, ahead = role(j, o)
        if o == 1:

            @pl.when(owns)
            def _():
                for d in range(2):
                    copy(*y_far(j, o, d)).start()

        @pl.when(jnp.logical_not(owns))
        def _():
            copy(*y_near(j, o, ahead, False)).start()

    def y4_far(j, o, d):
        rows, slot = pl.ds(64 * d, 64), YFIRST.index(j)
        return b["part"].at[j, o, :, rows], b["yfar4"].at[slot, feature(o)], b["y_s"].at[j, o], b["yf_r"].at[j, feature(o)], at_y(both[d])

    def y4_near(j, o, ahead, late):
        half = ahead if late else 1 - ahead
        rows = pl.ds(pl.multiple_of(64 * half, 64), 64)
        return (
            b["part"].at[j, o, :, rows],
            b["ynear4"].at[YFIRST.index(j), ahead, :, rows],
            b["y_s"].at[j, o],
            b["yn_r"].at[j],
            y_target(ahead),
        )

    def y_first_sends(j, o):
        owns, ahead = role(j, o)
        if o == 1:

            @pl.when(owns)
            def _():
                for d in range(2):
                    start(*y4_far(j, o, d))

        @pl.when(jnp.logical_not(owns))
        def _():
            start(*y4_near(j, o, ahead, False))

    def X0(j):
        @where_owned(j)
        def _():
            slot = YFIRST.index(j)
            landed(b["ynear4"].at[slot], b["yn_r"].at[j])
            b["part"][j, 0] = b["part"][j, 0] + (b["ynear4"][slot, 0] + b["ynear4"][slot, 1])
            far_sends(j, 0)
            I(j, 0)

    def Y1(j, o):
        owns, ahead = role(j, o)

        @pl.when(jnp.logical_not(owns))
        def _():
            if j in YFIRST:
                slot = YFIRST.index(j)
                landed(b["yfar4"].at[slot, feature(o)], b["yf_r"].at[j, feature(o)])
                rows = pl.ds(pl.multiple_of(64 * ahead, 64), 64)
                b["part"][j, o, :, rows] = b["part"][j, o, :, rows] + b["yfar4"][slot, feature(o)]
                start(*y4_near(j, o, ahead, True))
                return
            landed(b["yfar"].at[j, feature(o)], b["yf_r"].at[j, feature(o)])
            rows = pl.ds(pl.multiple_of(64 * ahead, 64), 64)
            b["summed"][j, o, rows] = b["summed"][j, o, rows] + b["yfar"][j, feature(o)]
            copy(*y_near(j, o, ahead, True)).start()

    def Y2(j):
        owns, _ = role(j, 0)

        @pl.when(owns)
        def _():
            landed(b["ynear"].at[j], b["yn_r"].at[j])
            put(j, b["summed"][j, 0] + (b["ynear"][j, 0] + b["ynear"][j, 1]))

    steps = dict(XO=XO, GC=GC, I=I, X0=X0, S=S, E=E, XS=XS, R=R, XA=XA, GS=GS, GX=GX, GY=GY, GZ=GZ, GA=GA, GO=GO, M=M, X1=X1, X2=X2, Y1=Y1, Y2=Y2)
    for name, *which in ORDER:
        steps[name](*which)

    landed(x_hbm.at[pl.ds(0, 2048), :], b["x1_s"])
    landed(b["xoth"], b["x2_s"])
    for sem, piece in enumerate((b["gain_c"].at[0], b["gain_x"].at[pl.ds(0, 3)], b["gain_y"].at[pl.ds(0, 3)])):
        landed(piece, b["g_s"].at[sem])
    for sem in (3, 4):
        landed(b["gain_a"].at[pl.ds(0, 7)], b["g_s"].at[sem])
    for j in range(8):
        landed(b["gbuf"].at[j, pl.ds(0, 7), 0], b["z_s"].at[j])
        landed(b["gbuf"].at[j, :, 0], b["d_s"].at[j])
        for o in range(2):
            if j not in YFIRST:
                landed(b["part"].at[j, o, pl.ds(0, 3)], b["u_s"].at[j, o])
            y_sent = b["part"].at[j, o] if j in YFIRST else b["summed"].at[j, o]
            if o == 1:
                landed(y_sent, b["y_s"].at[j, o])
                continue
            owns, _ = role(j, o)

            @pl.when(jnp.logical_not(owns))
            def _():
                landed(y_sent, b["y_s"].at[j, o])

            if j in YFIRST:

                @pl.when(owns)
                def _():
                    landed(b["part"].at[j, o, pl.ds(0, 3)], b["u_s"].at[j, o])


def finish(grad_ref, gain_ref, first_ref, second_ref, new_first_ref, new_second_ref, update_ref, gain_grad_ref):
    grad = grad_ref[...]
    new_first = beta_one * first_ref[...] + (1.0 - beta_one) * grad
    new_second = beta_two * second_ref[...] + (1.0 - beta_two) * grad * grad
    new_first_ref[...] = new_first
    new_second_ref[...] = new_second
    update_ref[...] = new_first / correct_one / (jnp.sqrt(new_second / correct_two) + epsilon)
    for i in range(8):
        for k in range(8):
            first = (i * 8 + k) * 128
            gain_grad_ref[0:1, first : first + 128] = gain_ref[i, k : k + 1, :] * 0.125


def shards(proj_in, kv_grad, normed, norm_grad, first_moment, second_moment):
    vmem = pl.BlockSpec(memory_space=pltpu.VMEM)
    mean_grad, gain = pl.pallas_call(
        exchange,
        out_shape=(jax.ShapeDtypeStruct((256, 256), jnp.float32), jax.ShapeDtypeStruct((8, 8, 128), jnp.float32)),
        in_specs=[pl.BlockSpec(memory_space=pltpu.HBM)] * 4,
        out_specs=(vmem, vmem),
        scratch_shapes=list(SCRATCH.values()),
        compiler_params=pltpu.CompilerParams(
            collective_id=0, has_side_effects=True, vmem_limit_bytes=VMEM_LIMIT
        ),
        name="exchange",
    )(proj_in[0], kv_grad[0], normed[0], norm_grad[0])
    block = jax.ShapeDtypeStruct((256, 256), jnp.float32)
    new_first, new_second, update, gain_grad = pl.pallas_call(
        finish,
        out_shape=(block, block, block, jax.ShapeDtypeStruct((1, 8192), jnp.float32)),
        in_specs=[vmem] * 4,
        out_specs=(vmem,) * 4,
        name="finish",
    )(mean_grad, gain, first_moment[0], second_moment[0])
    return (new_first[None], new_second[None], update[None], gain_grad)


def solution(mesh):
    finer = Mesh(mesh.devices.reshape(4, 2, 2, 8, 2), DP_TP)
    return jax.shard_map(
        shards,
        mesh=finer,
        in_specs=(
            P(None, DP, TP),
            P(None, DP_TP, None),
            P(None, DP_TP, None),
            P(None, DP_TP, None),
            P(None, TP, DP),
            P(None, TP, DP),
        ),
        out_specs=(P(None, TP, DP), P(None, TP, DP), P(None, TP, DP), P()),
        check_vma=False,
    )
```
